32 devices in a mesh: rep: 2 (over x), stretch: 2 (over core), tp: 8 (over z, y).
Axes of the slice: x: 2, y: 2, z: 4, core: 2. Of those that a mesh axis runs over, the one named last changes fastest.
Arguments:
- query: bfloat16 [4, 512, 3072], P(('rep', 'stretch'), 'tp'), parts along dimension 0, may hold values from -64 to 64
- stretch_kv: bfloat16 [2, 4, 512, 3072], P(None, ('rep', 'stretch'), 'tp'), parts along dimension 1, may hold values from -6 to 6
- history_kv: bfloat16 [2, 4096, 3072], P(None, ('rep', 'tp')), parts along dimension 1, may hold values from -6 to 6
- block_mask: int32 [4, 4, 8], P(('rep', 'stretch')), parts along dimension 0, may hold values from 0 to 1, as said below
- noise_level: int32 [4], P(('rep', 'stretch')), parts along dimension 0, may hold values from 0 to 999
- history_blocks: int32 [2], P('rep'), parts along dimension 0, may hold values from 1 to 16
- out_weight: bfloat16 [3072, 6144], P(None, 'tp'), may hold values from -0.109375 to 0.109375
- gate_table: float32 [1000, 6144], P(None, 'tp'), may hold values from -6 to 6
Outputs:
- mixed: bfloat16 [4, 512, 6144], P(('rep', 'stretch'), None, 'tp'), parts along dimension 0
The draws below stay inside these ranges and needn't reach their ends.
There are 2 independent parts, one for each index of `rep`. The reference program is written for one: setup_inputs(seed, part) draws one part's arguments, and reference() takes and returns one part's arrays. A program takes and returns all parts, laid end to end along the dimension named above; an argument that names none is the same for every part. Nothing has to cross between parts.
Inputs may be any that keep to these rules, and one draw needn't show every extreme that they name: block_mask[c, i, 4 + i] = 1 for every query block i; block_mask[0, i, j] = 0 for j < 4.
All inputs are finite; a program needn't handle non-finite values.
Results may differ from the reference program's by a relative error of at most 0.0049.
Values may be sent and summed in bfloat16 or wider, within the bound.
No kernel may reach another device: no remote copies, remote signals or barrier semaphores. Data moves between devices by JAX's collectives and lax.ppermute only.
A program may use at most 128 MiB of HBM per device.

```python
import math
import jax
import jax.numpy as jnp
from jax import lax

D = 6144
H = 24
HD = 128
LEVELS = 1000
BLK = 128
CT = 512
QB = 4
HIST = 2048


def shared_draws(key):
    query_key = jax.random.fold_in(key, 101)
    history_key = jax.random.fold_in(key, 202)
    feature_width = H * HD
    history = jnp.clip(jax.random.normal(history_key, (2, HIST, feature_width), jnp.float32), -6.0, 6.0)
    queries = jnp.clip(2.0 * jax.random.normal(query_key, (2, CT, feature_width), jnp.float32), -12.0, 12.0)
    return (queries, history)


def draw_query(key, part):
    return shared_draws(key)[0].astype(jnp.bfloat16)


def draw_history_kv(key, part):
    return shared_draws(key)[1].astype(jnp.bfloat16)


def draw_block_mask(key, part):
    raw_bits = jax.random.randint(jax.random.fold_in(key, 404), (2, QB, 2 * QB), 0, 5)
    grid_rows = lax.broadcasted_iota(jnp.int32, (2, QB, 2 * QB), 1)
    grid_cols = lax.broadcasted_iota(jnp.int32, (2, QB, 2 * QB), 2)
    grid_stretches = lax.broadcasted_iota(jnp.int32, (2, QB, 2 * QB), 0)
    block_allow = jnp.where(raw_bits < 3, 1, 0)
    block_allow = jnp.where(grid_cols == grid_rows + QB, 1, block_allow)
    block_allow = jnp.where((grid_stretches == 0) & (grid_cols < QB), 0, block_allow)
    return block_allow.astype(jnp.int32)


def levels(rng, extent, shards, least, high):
    level = 1.0
    for position, parts in shards:
        heights = jax.random.uniform(jax.random.fold_in(jax.random.fold_in(rng, 6), position), (parts,), jnp.float32, least / len(shards), high / len(shards))
        level = level * jnp.repeat(jnp.exp(heights), extent[position] // parts).reshape((-1,) + (1,) * (len(extent) - 1 - position))
    return level


def bell_draw(own_key, dims, width, most, shards=(), kind=jnp.bfloat16):
    values = jax.random.normal(own_key, dims, jnp.float32) * width
    if len(shards) > 0:
        values = levels(own_key, dims, shards, -0.22, 0.18) * values
    return jnp.clip(values, min=-most, max=most).astype(kind)


def setup_inputs(seed: int = 0, part: int = 0) -> dict:
    key_list = jax.random.split(jax.random.key(seed), 9)
    own_keys = jax.random.split(jax.random.fold_in(key_list[8], part), 9)
    return {
        "query": draw_query(jax.random.fold_in(jax.random.fold_in(key_list[8], part), 71), part),
        "stretch_kv": bell_draw(own_keys[1], (2, 2, CT, H * HD), 1.0, 6.0, ((1, 2), (2, 8))),
        "history_kv": draw_history_kv(jax.random.fold_in(jax.random.fold_in(key_list[8], part), 71), part),
        "block_mask": draw_block_mask(jax.random.fold_in(jax.random.fold_in(key_list[8], part), 71), part),
        "noise_level": jax.random.randint(own_keys[4], (2,), 0, LEVELS).astype(jnp.int32),
        "history_blocks": jax.random.randint(own_keys[5], (1,), 1, HIST // BLK + 1).astype(jnp.int32),
        "out_weight": bell_draw(key_list[6], (H * HD, D), (H * HD) ** -0.5, 0.109375, ((1, 8),)),
        "gate_table": bell_draw(key_list[7], (LEVELS, D), 1.0, 6.0, ((1, 8),), jnp.float32),
    }


NEGATIVE = -1e+30

def single_head(triple_args, allowed):
    queries, key_rows, value_rows = triple_args
    scores = jnp.dot(queries, key_rows.T, preferred_element_type=jnp.float32) * (1.0 / math.sqrt(HD))
    scores = jnp.where(allowed, scores, NEGATIVE)
    row_peak = lax.optimization_barrier(jnp.max(scores, axis=1, keepdims=True))
    weights = jnp.where(allowed, jnp.exp(scores - row_peak), 0.0)
    weight_sum = lax.optimization_barrier(jnp.sum(weights, axis=1, keepdims=True))
    output = jnp.dot(weights, value_rows.astype(jnp.float32), precision=lax.Precision.HIGHEST) / weight_sum
    return output.astype(jnp.bfloat16)

def reference(query, stretch_kv, history_kv, block_mask, noise_level, history_blocks, out_weight, gate_table):
    history_live = jnp.arange(HIST, dtype=jnp.int32) < history_blocks[0] * BLK
    results = []
    for stretch_index in range(2):
        if stretch_index == 1:
            older_pair = stretch_kv[:, 0]
        else:
            older_pair = jnp.zeros_like(stretch_kv[:, 0])
        key_rows = jnp.concatenate([history_kv[0], older_pair[0], stretch_kv[0, stretch_index]], 0)
        value_rows = jnp.concatenate([history_kv[1], older_pair[1], stretch_kv[1, stretch_index]], 0)
        fresh = jnp.repeat(jnp.repeat(block_mask[stretch_index] > 0, BLK, axis=0), BLK, axis=1)
        allowed = jnp.concatenate([jnp.broadcast_to(history_live[None, :], (CT, HIST)), fresh], 1)
        key_count = key_rows.shape[0]
        head_queries = jnp.transpose(query[stretch_index].reshape(CT, H, HD), (1, 0, 2))
        head_keys = jnp.transpose(key_rows.reshape(key_count, H, HD), (1, 0, 2))
        head_values = jnp.transpose(value_rows.reshape(key_count, H, HD), (1, 0, 2))
        attended = lax.map(lambda triple_args: single_head(triple_args, allowed), (head_queries, head_keys, head_values))
        attended = jnp.transpose(attended, (1, 0, 2)).reshape(CT, H * HD)
        projected = jnp.dot(attended, out_weight, preferred_element_type=jnp.float32)
        gate_row = gate_table[noise_level[stretch_index]]
        results.append((projected * gate_row[None, :]).astype(jnp.bfloat16))
    return jnp.stack(results, 0)
```

```python
import functools
import math

import jax
import jax.numpy as jnp
from jax import lax
from jax.experimental import pallas as pl
from jax.experimental.pallas import tpu as pltpu
from jax.sharding import PartitionSpec as P

HD = 128
BLK = 128
NEGATIVE = -1e30
LOG2_SCALE = math.log2(math.e) / math.sqrt(HD)


def head_groups(head_count, tp_count):
    both = math.gcd(head_count, tp_count)
    return both & -both


def xor_permute(value, group, step):
    count = lax.axis_size("tp")
    pairs = [(t, (t // group) * group + ((t % group) ^ step)) for t in range(count)]
    return lax.ppermute(value, "tp", pairs)


def partner_core(value):
    return lax.ppermute(value, "stretch", [(0, 1), (1, 0)])


def attention_body(place, q_ref, own_ref, other_ref, bias_ref, out_ref, *rest, rows, half, heads):
    stats = rest[:-1]
    q_scr = rest[-1]
    outer, group = q_ref.shape[0], q_ref.shape[1]
    for o in range(outer):
        for t in range(group):
            q_scr[pl.ds((o * group + t) * rows, rows), :] = q_ref[o, place[0] ^ t]
    total_rows = outer * group * rows
    block_count = bias_ref.shape[0]
    q_block = total_rows // block_count

    def flat(ref, low, count, h):
        part = ref[:, low : low + count, h * HD : (h + 1) * HD]
        return part.reshape(group * count, HD)

    for h in range(heads):
        queries = q_scr[:, h * HD : (h + 1) * HD]
        peak = total = acc = None
        column = 0
        for ref, low, count, value_low in (
            (own_ref, 2 * half, rows, 2 * half + rows),
            (other_ref, 2 * half, rows, 2 * half + rows),
            (own_ref, 0, half, half),
            (other_ref, 0, half, half),
        ):
            keys = flat(ref, low, count, h)
            values = flat(ref, value_low, count, h)
            width = keys.shape[0]
            scores = lax.dot_general(
                queries, keys, (((1,), (1,)), ((), ())), preferred_element_type=jnp.float32
            )
            scores = scores.reshape(block_count, q_block, width) * LOG2_SCALE
            scores = scores + bias_ref[:, :, column : column + width]
            scores = scores.reshape(total_rows, width)
            column += width
            top = jnp.max(scores, axis=1, keepdims=True)
            new_peak = top if peak is None else jnp.maximum(peak, top)
            weights = jnp.exp2(scores - new_peak)
            part = jnp.sum(weights, axis=1, keepdims=True)
            product = jnp.dot(
                weights.astype(jnp.bfloat16), values, preferred_element_type=jnp.float32
            )
            if peak is None:
                total, acc = part, product
            else:
                scale = jnp.exp2(peak - new_peak)
                total = total * scale + part
                acc = acc * scale + product
            peak = new_peak
        cols = slice(h * HD, (h + 1) * HD)
        if stats:
            out_ref[:, cols] = acc
            stats[0][:, h : h + 1] = peak
            stats[1][:, h : h + 1] = total
        else:
            out_ref[:, cols] = (acc / total).astype(out_ref.dtype)


def attention(place, q, own, other, bias, rows, half, partial):
    heads = q.shape[-1] // HD
    total_rows = q.shape[0] * q.shape[1] * rows
    wide = jax.ShapeDtypeStruct((total_rows, heads * HD), jnp.float32 if partial else jnp.bfloat16)
    thin = jax.ShapeDtypeStruct((total_rows, heads), jnp.float32)
    vmem = pl.BlockSpec(memory_space=pltpu.VMEM)
    return pl.pallas_call(
        functools.partial(attention_body, rows=rows, half=half, heads=heads),
        out_shape=(wide, thin, thin) if partial else wide,
        in_specs=[pl.BlockSpec(memory_space=pltpu.SMEM)] + [vmem] * 4,
        out_specs=(vmem,) * 3 if partial else vmem,
        scratch_shapes=[pltpu.VMEM((total_rows, heads * HD), jnp.bfloat16)],
        name="attend",
    )(place, q, own, other, bias)


def project_body(place, parts_ref, weight_ref, gate_ref, out_ref):
    group, _, width = parts_ref.shape
    acc = None
    for step in range(group):
        low = pl.multiple_of((place[0] ^ step) * width, width)
        product = jnp.dot(
            parts_ref[step], weight_ref[pl.ds(low, width), :], preferred_element_type=jnp.float32
        )
        acc = product if acc is None else acc + product
    out_ref[...] = (acc * gate_ref[...]).astype(out_ref.dtype)


def project(place, parts, weight, gate_row):
    vmem = pl.BlockSpec(memory_space=pltpu.VMEM)
    return pl.pallas_call(
        project_body,
        out_shape=jax.ShapeDtypeStruct((parts.shape[1], weight.shape[1]), jnp.bfloat16),
        in_specs=[pl.BlockSpec(memory_space=pltpu.SMEM)] + [vmem] * 3,
        out_specs=vmem,
        name="project",
    )(place, parts, weight, gate_row)


def key_bias(block_mask, live_limit, sources, rows, half, history_rows, core):
    block_count = block_mask.shape[0]
    fresh = (sources[:, None] * rows + jnp.arange(rows, dtype=jnp.int32)[None, :]).reshape(-1) // BLK
    hot = fresh[:, None] == jnp.arange(block_count, dtype=jnp.int32)[None, :]
    mask = block_mask > 0

    def fresh_part(columns):
        return jnp.any(hot[None, :, :] & columns[:, None, :], axis=2)

    def history_part(which):
        base = sources[:, None] * history_rows + which * half
        position = (base + jnp.arange(half, dtype=jnp.int32)[None, :]).reshape(-1)
        return jnp.broadcast_to((position < live_limit)[None, :], (block_count, position.shape[0]))

    allowed = jnp.concatenate(
        [
            fresh_part(mask[:, block_count:]),
            fresh_part(mask[:, :block_count]),
            history_part(core),
            history_part(1 - core),
        ],
        axis=1,
    )
    return jnp.where(allowed, 0.0, NEGATIVE).astype(jnp.float32)[:, None, :]


def on_device(
    query, stretch_kv, history_kv, block_mask, noise_level, history_blocks, out_weight, gate_table
):
    tp_count = lax.axis_size("tp")
    tp_index = lax.axis_index("tp")
    core = lax.axis_index("stretch")
    rows = query.shape[1]
    feature_width = query.shape[2]
    history_rows = history_kv.shape[1]
    half = history_rows // 2
    group = head_groups(feature_width // HD, tp_count)
    outer = tp_count // group
    width = feature_width // group
    member = tp_index % group
    base = tp_index - member
    place = member[None].astype(jnp.int32)

    history_half = lax.dynamic_slice_in_dim(history_kv, core * half, half, axis=1)
    stacked = jnp.concatenate(
        [history_half[0], history_half[1], stretch_kv[0, 0], stretch_kv[1, 0], query[0]], axis=0
    )
    kv_rows = 2 * half + 2 * rows

    def block_for(step):
        return lax.dynamic_slice_in_dim(stacked, (member ^ step) * width, width, axis=1)

    order = sorted(range(1, group), reverse=True)
    received = {0: block_for(0)}
    for step in order:
        received[step] = xor_permute(block_for(step), group, step)
    own = jnp.stack([received[step] for step in range(group)])
    other = partner_core(own[:, :kv_rows])
    q = own[None, :, kv_rows:]
    if outer > 1:
        same = [[o * group + m for o in range(outer)] for m in range(group)]
        q = lax.all_gather(q[0], "tp", axis=0, axis_index_groups=same)

    sources = base + (member ^ jnp.arange(group, dtype=jnp.int32))
    bias = key_bias(
        block_mask[0], history_blocks[0] * BLK, sources, rows, half, history_rows, core
    )
    if outer > 1:
        out, peak, total = attention(place, q, own, other, bias, rows, half, True)
        outs = lax.all_gather(out, "tp", axis=0, axis_index_groups=same)
        peaks = lax.all_gather(peak, "tp", axis=0, axis_index_groups=same)
        totals = lax.all_gather(total, "tp", axis=0, axis_index_groups=same)
        factor = jnp.exp2(peaks - jnp.max(peaks, axis=0, keepdims=True))
        total = jnp.sum(totals * factor, axis=0)
        heads = width // HD
        outs = outs.reshape(outer, -1, heads, HD) * factor[..., None]
        attended = (jnp.sum(outs, axis=0) / total[..., None]).astype(jnp.bfloat16)
        attended = attended.reshape(-1, width)
    else:
        attended = attention(place, q, own, other, bias, rows, half, False)

    parts = {0: attended}
    for step in range(group - 2, 0, -2):
        parts[step] = xor_permute(attended, group, step)
    for step in range(0, group, 2):
        parts[step + 1] = xor_permute(parts[step], group, 1)
    gathered = jnp.stack([parts[step] for step in range(group)])
    gate_row = lax.dynamic_slice_in_dim(gate_table, noise_level[0], 1, axis=0)
    return project(place, gathered, out_weight, gate_row)[None]


def solution(mesh):
    return jax.shard_map(
        on_device,
        mesh=mesh,
        in_specs=(
            P(("rep", "stretch"), "tp", None),
            P(None, ("rep", "stretch"), "tp", None),
            P(None, ("rep", "tp"), None),
            P(("rep", "stretch"), None, None),
            P(("rep", "stretch")),
            P("rep"),
            P(None, "tp"),
            P(None, "tp"),
        ),
        out_specs=P(("rep", "stretch"), None, "tp"),
        check_vma=False,
    )
```

```python
import functools
import math

import jax
import jax.numpy as jnp
from jax import lax
from jax.experimental import pallas as pl
from jax.experimental.pallas import tpu as pltpu
from jax.sharding import PartitionSpec as P


HD = 128
BLK = 128
NEGATIVE = -1e30
LOG2_SCALE = math.log2(math.e) / math.sqrt(HD)
CHUNKS = 2

VMEM = pl.BlockSpec(memory_space=pltpu.VMEM)
SMEM = pl.BlockSpec(memory_space=pltpu.SMEM)
HBM = pl.BlockSpec(memory_space=pltpu.HBM)


def head_groups(head_count, tp_count):
    both = math.gcd(head_count, tp_count)
    return both & -both


def head_chunks(heads, count):
    count = min(count, heads)
    sizes = [heads // count + (1 if i < heads % count else 0) for i in range(count)]
    return [(sum(sizes[:i]), sizes[i]) for i in range(count)]


def xor_permute(value, group, step, senders=None):
    count = lax.axis_size("tp")
    pairs = [
        (t, (t // group) * group + ((t % group) ^ step))
        for t in range(count)
        if senders is None or t % group in senders
    ]
    return lax.ppermute(value, "tp", pairs)


def spread(value, member, group):
    def send(block, step, senders=None):
        return xor_permute(block, group, step, senders)

    if group == 1:
        return [value], [member]
    line = [(value, member)]
    if group == 8:
        over = send(value, 4)
        line += [(send(value, 2), member ^ 2), (over, member ^ 4)]
        line += [(send(over, 2), member ^ 6)]
    else:
        line += [(send(value, step), member ^ step) for step in range(2, group, 2)]
    across = [(send(block, 1), source ^ 1) for block, source in line]
    blocks, members = zip(*(line + across))
    return list(blocks), list(members)


def partner_core(value):
    return lax.ppermute(value, "stretch", [(0, 1), (1, 0)])


def pack_body(place, query, stretch, history, *rest, half, rows, width, plan):
    count = len(plan)
    blocks, stages = rest[:count], rest[count : 2 * count]
    in_sems, out_sems = rest[2 * count :]
    row = pl.multiple_of(place[1] * half, 8)
    incoming = []
    for index, (step, low, cols) in enumerate(plan):
        column = pl.ds(pl.multiple_of((place[0] ^ step) * width + low, HD), cols)
        parts = (
            (history.at[0, pl.ds(row, half), column], 0, half),
            (history.at[1, pl.ds(row, half), column], half, half),
            (stretch.at[0, :, column], 2 * half, rows),
            (stretch.at[1, :, column], 2 * half + rows, rows),
            (query.at[:, column], 2 * half + 2 * rows, rows),
        )
        copies = [
            pltpu.make_async_copy(
                source, stages[index].at[pl.ds(at, size), :], in_sems.at[index, part]
            )
            for part, (source, at, size) in enumerate(parts)
        ]
        for copy in copies:
            copy.start()
        incoming.append(copies)
    outgoing = []
    for index, copies in enumerate(incoming):
        for copy in copies:
            copy.wait()
        copy = pltpu.make_async_copy(stages[index], blocks[index], out_sems.at[index])
        copy.start()
        outgoing.append(copy)
    for copy in outgoing:
        copy.wait()


def pack(place, query, stretch, history, width, plan):
    rows, half = query.shape[0], history.shape[1] // 2
    shapes = [(2 * half + 3 * rows, cols) for _, _, cols in plan]
    return pl.pallas_call(
        functools.partial(pack_body, half=half, rows=rows, width=width, plan=plan),
        out_shape=tuple(jax.ShapeDtypeStruct(shape, query.dtype) for shape in shapes),
        in_specs=[SMEM, HBM, HBM, HBM],
        out_specs=(HBM,) * len(plan),
        scratch_shapes=[pltpu.VMEM(shape, query.dtype) for shape in shapes]
        + [
            pltpu.SemaphoreType.DMA((len(plan), 5)),
            pltpu.SemaphoreType.DMA((len(plan),)),
        ],
        name="pack",
    )(place, query, stretch, history)


def attention_body(place, bias_ref, *rest, rows, half, heads, low, inner, outer, group, partial):
    kv_rows = 2 * half + 2 * rows
    refs, rest = rest[:group], rest[group:]
    own = [(ref, 0, low if step < inner else 0) for step, ref in enumerate(refs)]
    other = [(rest[0], step * kv_rows, low) for step in range(inner)]
    rest = rest[1:]
    if inner < group:
        other += [(rest[0], step * kv_rows, 0) for step in range(group - inner)]
        rest = rest[1:]
    q_all = None
    if partial:
        q_all, rest = rest[0], rest[1:]
    out_ref, stats, q_scr = rest[0], rest[1:-1], rest[-1]
    for step, (ref, _, base) in enumerate(own):
        member = place[0] ^ step
        for o in range(outer):
            at = pl.multiple_of((o * group + member) * rows, 8)
            if partial:
                q_scr[pl.ds(at, rows), :] = q_all[o, step]
            else:
                q_scr[pl.ds(at, rows), :] = ref[kv_rows:, base : base + heads * HD]
    total_rows = outer * group * rows
    block_count = bias_ref.shape[0]
    q_block = total_rows // block_count

    for h in range(heads):
        cols = slice(h * HD, (h + 1) * HD)
        queries = q_scr[:, cols]

        def flat(sources, first, count):
            pieces = []
            for ref, row, base in sources:
                columns = slice(base + h * HD, base + (h + 1) * HD)
                pieces.append(ref[row + first : row + first + count, columns])
            return jnp.concatenate(pieces, axis=0)

        peak = total = acc = None
        column = 0
        for sources, first, count, value_first in (
            (own, 2 * half, rows, 2 * half + rows),
            (other, 2 * half, rows, 2 * half + rows),
            (own, 0, half, half),
            (other, 0, half, half),
        ):
            keys = flat(sources, first, count)
            values = flat(sources, value_first, count)
            width = keys.shape[0]
            scores = lax.dot_general(
                queries, keys, (((1,), (1,)), ((), ())), preferred_element_type=jnp.float32
            )
            scores = scores.reshape(block_count, q_block, width) * LOG2_SCALE
            scores = scores + bias_ref[:, :, column : column + width]
            scores = scores.reshape(total_rows, width)
            column += width
            top = jnp.max(scores, axis=1, keepdims=True)
            new_peak = top if peak is None else jnp.maximum(peak, top)
            weights = jnp.exp2(scores - new_peak)
            part = jnp.sum(weights, axis=1, keepdims=True)
            product = jnp.dot(
                weights.astype(jnp.bfloat16), values, preferred_element_type=jnp.float32
            )
            if peak is None:
                total, acc = part, product
            else:
                scale = jnp.exp2(peak - new_peak)
                total = total * scale + part
                acc = acc * scale + product
            peak = new_peak
        if partial:
            out_ref[:, cols] = acc
            stats[0][:, h : h + 1] = peak
            stats[1][:, h : h + 1] = total
        else:
            out_ref[:, cols] = (acc / total).astype(out_ref.dtype)


def attention(place, bias, own, others, q_all, rows, half, total_rows, low, cols):
    group = len(own)
    partial = q_all is not None
    wide = jax.ShapeDtypeStruct((total_rows, cols), jnp.float32 if partial else jnp.bfloat16)
    thin = jax.ShapeDtypeStruct((total_rows, cols // HD), jnp.float32)
    body = functools.partial(
        attention_body,
        rows=rows,
        half=half,
        heads=cols // HD,
        low=low,
        inner=max(group // 2, 1),
        outer=total_rows // (group * rows),
        group=group,
        partial=partial,
    )
    operands = (*own, *others) + ((q_all,) if partial else ())
    return pl.pallas_call(
        body,
        out_shape=(wide, thin, thin) if partial else wide,
        in_specs=[SMEM] + [VMEM] * (1 + len(operands)),
        out_specs=(VMEM,) * 3 if partial else VMEM,
        scratch_shapes=[pltpu.VMEM((total_rows, cols), jnp.bfloat16)],
        compiler_params=pltpu.CompilerParams(vmem_limit_bytes=24 << 20),
        name="attend",
    )(place, bias, *operands)


def project_body(starts, place, weight, *rest, group, low, last, first):
    parts, rest = rest[:group], rest[group:]
    cols = parts[0].shape[1]
    left = jnp.concatenate([part[...] for part in parts], axis=1)
    right = jnp.concatenate(
        [
            weight[pl.ds(pl.multiple_of(starts[step] + low, HD), cols), :]
            for step in range(group)
        ],
        axis=0,
    )
    acc = jnp.dot(left, right, preferred_element_type=jnp.float32)
    if not first:
        acc = acc + rest[0][...]
        rest = rest[1:]
    if last:
        gate, out = rest
        acc = acc * gate[pl.ds(place[2] % 8, 1), :]
    else:
        (out,) = rest
    out[...] = acc.astype(out.dtype)


def project(starts, place, parts, weight, before, gate, low):
    group = len(parts)
    first, last = before is None, gate is not None
    operands = [weight, *parts]
    operands += [] if first else [before]
    operands += [gate] if last else []
    shape = (parts[0].shape[0], weight.shape[1])
    return pl.pallas_call(
        functools.partial(
            project_body, group=group, low=low, last=last, first=first
        ),
        out_shape=jax.ShapeDtypeStruct(shape, jnp.bfloat16 if last else jnp.float32),
        in_specs=[SMEM, SMEM] + [VMEM] * len(operands),
        out_specs=VMEM,
        compiler_params=pltpu.CompilerParams(vmem_limit_bytes=24 << 20),
        name="project",
    )(starts, place, *operands)


def pick_body(place, table, out, sem):
    row = pl.multiple_of(place[2] // 8 * 8, 8)
    copy = pltpu.make_async_copy(table.at[pl.ds(row, 8), :], out, sem)
    copy.start()
    copy.wait()


def pick_gate(place, table):
    return pl.pallas_call(
        pick_body,
        out_shape=jax.ShapeDtypeStruct((8, table.shape[1]), table.dtype),
        in_specs=[SMEM, HBM],
        out_specs=VMEM,
        scratch_shapes=[pltpu.SemaphoreType.DMA],
        compiler_params=pltpu.CompilerParams(vmem_limit_bytes=1 << 20),
        name="pick",
    )(place, table)


def key_bias(block_mask, live_limit, sources, rows, half, history_rows, core):
    block_count = block_mask.shape[0]
    fresh = (sources[:, None] * rows + jnp.arange(rows, dtype=jnp.int32)[None, :]).reshape(-1) // BLK
    hot = fresh[:, None] == jnp.arange(block_count, dtype=jnp.int32)[None, :]
    mask = block_mask > 0

    def fresh_part(columns):
        return jnp.any(hot[None, :, :] & columns[:, None, :], axis=2)

    def history_part(which):
        base = sources[:, None] * history_rows + which * half
        position = (base + jnp.arange(half, dtype=jnp.int32)[None, :]).reshape(-1)
        return jnp.broadcast_to((position < live_limit)[None, :], (block_count, position.shape[0]))

    allowed = jnp.concatenate(
        [
            fresh_part(mask[:, block_count:]),
            fresh_part(mask[:, :block_count]),
            history_part(core),
            history_part(1 - core),
        ],
        axis=1,
    )
    return jnp.where(allowed, 0.0, NEGATIVE).astype(jnp.float32)[:, None, :]


def on_device(
    query, stretch_kv, history_kv, block_mask, noise_level, history_blocks, out_weight, gate_table
):
    tp_count = lax.axis_size("tp")
    tp_index = lax.axis_index("tp")
    core = lax.axis_index("stretch")
    rows = query.shape[1]
    feature_width = query.shape[2]
    history_rows = history_kv.shape[1]
    half = history_rows // 2
    group = head_groups(feature_width // HD, tp_count)
    outer = tp_count // group
    width = feature_width // group
    total_rows = tp_count * rows
    member = tp_index % group
    kv_rows = 2 * half + 2 * rows
    place = jnp.stack([member, core, noise_level[0]]).astype(jnp.int32)
    same = [[o * group + m for o in range(outer)] for m in range(group)]
    chunks = [(low * HD, count * HD) for low, count in head_chunks(width // HD, CHUNKS)]

    sources = tp_index - member + (member ^ jnp.arange(group, dtype=jnp.int32))
    bias = key_bias(
        block_mask[0], history_blocks[0] * BLK, sources, rows, half, history_rows, core
    )

    inner = max(group // 2, 1)
    cross = list(range(group - 1, inner - 1, -1))
    plan = [(step, low, cols) for low, cols in chunks[:1] for step in cross]
    plan += [(step, 0, width) for step in range(inner)]
    plan += [(step, low, cols) for low, cols in chunks[1:] for step in cross]
    blocks = pack(place, query[0], stretch_kv[:, 0], history_kv, width, plan)
    sends = [{} for _ in chunks]
    near = {}
    for (step, low, cols), block in zip(plan, blocks):
        if step >= inner:
            index = [first for first, _ in chunks].index(low)
            sends[index][step] = xor_permute(block, group, step)
        elif step == 0:
            near[step] = block
        else:
            near[step] = xor_permute(block, group, step)
    other_near = partner_core(
        jnp.concatenate([near[step][:kv_rows] for step in range(inner)], axis=0)
    )

    gathered = []
    for index, (low, cols) in enumerate(chunks):
        far = sends[index]
        own = [near[step] for step in range(inner)] + [far[step] for step in reversed(cross)]
        others = [other_near]
        if cross:
            others.append(
                partner_core(
                    jnp.concatenate([far[step][:kv_rows] for step in reversed(cross)], axis=0)
                )
            )
        attend = functools.partial(
            attention,
            place,
            bias,
            own,
            others,
            rows=rows,
            half=half,
            total_rows=total_rows,
            low=low,
            cols=cols,
        )
        if outer > 1:
            q = jnp.stack(
                [
                    block[kv_rows:, low : low + cols] if step < inner else block[kv_rows:]
                    for step, block in enumerate(own)
                ]
            )
            q = lax.all_gather(q, "tp", axis=0, axis_index_groups=same)
            out, peak, total = attend(q_all=q)
            outs, peaks, totals = (
                lax.all_gather(value, "tp", axis=0, axis_index_groups=same)
                for value in (out, peak, total)
            )
            factor = jnp.exp2(peaks - jnp.max(peaks, axis=0, keepdims=True))
            total = jnp.sum(totals * factor, axis=0)
            outs = outs.reshape(outer, total_rows, -1, HD) * factor[..., None]
            attended = (jnp.sum(outs, axis=0) / total[..., None]).astype(jnp.bfloat16)
            attended = attended.reshape(total_rows, -1)
        else:
            attended = attend(q_all=None)
        parts, members = spread(attended, member, group)
        gathered.append(parts)
    starts = (jnp.stack(members) * width).astype(jnp.int32)

    gate_rows = pick_gate(place, gate_table)
    result = None
    for index, ((low, _), parts) in enumerate(zip(chunks, gathered)):
        gate = gate_rows if index == len(chunks) - 1 else None
        result = project(starts, place, parts, out_weight, result, gate, low)
    return result[None]


def solution(mesh):
    return jax.shard_map(
        on_device,
        mesh=mesh,
        in_specs=(
            P(("rep", "stretch"), "tp", None),
            P(None, ("rep", "stretch"), "tp", None),
            P(None, ("rep", "tp"), None),
            P(("rep", "stretch"), None, None),
            P(("rep", "stretch")),
            P("rep"),
            P(None, "tp"),
            P(None, "tp"),
        ),
        out_specs=P(("rep", "stretch"), None, "tp"),
        check_vma=False,
    )
```

```python
import functools
import math

import jax
import jax.numpy as jnp
from jax import lax
from jax.experimental import pallas as pl
from jax.experimental.pallas import tpu as pltpu
from jax.sharding import PartitionSpec as P


HD = 128
BLK = 128
NEGATIVE = -1e30
LOG2_SCALE = math.log2(math.e) / math.sqrt(HD)
CHUNKS = 2
VMEM_LIMIT = 12 << 20

VMEM = pl.BlockSpec(memory_space=pltpu.VMEM)
SMEM = pl.BlockSpec(memory_space=pltpu.SMEM)
HBM = pl.BlockSpec(memory_space=pltpu.HBM)


def head_groups(head_count, tp_count):
    both = math.gcd(head_count, tp_count)
    return both & -both


def head_chunks(heads, count):
    count = min(count, heads)
    sizes = [heads // count + (1 if i < heads % count else 0) for i in range(count)]
    return [(sum(sizes[:i]), sizes[i]) for i in range(count)]


def xor_permute(value, group, step, senders=None):
    count = lax.axis_size("tp")
    pairs = [
        (t, (t // group) * group + ((t % group) ^ step))
        for t in range(count)
        if senders is None or t % group in senders
    ]
    return lax.ppermute(value, "tp", pairs)


def spread(value, heads, group):
    def send(block, step):
        return xor_permute(block, group, step)

    def both(block, step):
        return [(block, step), (send(block, 1), step ^ 1)]

    if group == 1:
        return [(value, 0)], [[] for _ in heads]
    near = both(value, 0)
    if group == 8:
        near += both(send(value, 2), 2)
    far = []
    for block in heads:
        pieces = []
        if group == 8:
            over = send(block, 4)
            pieces += both(over, 4)
            pieces += both(send(over, 2), 6)
        else:
            for step in range(2, group, 2):
                moved = send(block, step)
                pieces += both(moved, step)
        far.append(pieces)
    return near, far


def partner_core(value):
    return lax.ppermute(value, "stretch", [(0, 1), (1, 0)])


def pack_body(place, *rest, half, rows, width, plan, gated):
    if gated:
        table, rest = rest[0], rest[1:]
    query, stretch, history, rest = *rest[:3], rest[3:]
    count = len(plan)
    if gated:
        gate_out, rest = rest[0], rest[1:]
        gate_sem, rest = rest[-1], rest[:-1]
        gate_row = pl.multiple_of(place[2] // 8 * 8, 8)
        gate_copy = pltpu.make_async_copy(table.at[pl.ds(gate_row, 8), :], gate_out, gate_sem)
        gate_copy.start()
    blocks, stages = rest[:count], rest[count : 2 * count]
    in_sems, out_sems = rest[2 * count :]
    row = pl.multiple_of(place[1] * half, 8)
    incoming = []
    for index, (step, low, cols) in enumerate(plan):
        column = pl.ds(pl.multiple_of((place[0] ^ step) * width + low, HD), cols)
        parts = (
            (history.at[0, pl.ds(row, half), column], 0, half),
            (history.at[1, pl.ds(row, half), column], half, half),
            (stretch.at[0, :, column], 2 * half, rows),
            (stretch.at[1, :, column], 2 * half + rows, rows),
            (query.at[:, column], 2 * half + 2 * rows, rows),
        )
        copies = [
            pltpu.make_async_copy(
                source, stages[index].at[pl.ds(at, size), :], in_sems.at[index, part]
            )
            for part, (source, at, size) in enumerate(parts)
        ]
        for copy in copies:
            copy.start()
        incoming.append(copies)
    outgoing = []
    for index, copies in enumerate(incoming):
        for copy in copies:
            copy.wait()
        copy = pltpu.make_async_copy(stages[index], blocks[index], out_sems.at[index])
        copy.start()
        outgoing.append(copy)
    for copy in outgoing:
        copy.wait()
    if gated:
        gate_copy.wait()


def pack(place, query, stretch, history, width, plan, table=None):
    gated = table is not None
    rows, half = query.shape[0], history.shape[1] // 2
    shapes = [(2 * half + 3 * rows, cols) for _, _, cols in plan]
    outs = [jax.ShapeDtypeStruct(shape, query.dtype) for shape in shapes]
    scratch = [pltpu.VMEM(shape, query.dtype) for shape in shapes]
    scratch += [pltpu.SemaphoreType.DMA((len(plan), 5)), pltpu.SemaphoreType.DMA((len(plan),))]
    operands = [query, stretch, history]
    out_specs = [HBM] * len(plan)
    if gated:
        outs = [jax.ShapeDtypeStruct((8, table.shape[1]), table.dtype)] + outs
        out_specs = [VMEM] + out_specs
        scratch.append(pltpu.SemaphoreType.DMA)
        operands = [table] + operands
    return pl.pallas_call(
        functools.partial(
            pack_body, half=half, rows=rows, width=width, plan=plan, gated=gated
        ),
        out_shape=tuple(outs),
        in_specs=[SMEM] + [HBM] * len(operands),
        out_specs=tuple(out_specs),
        scratch_shapes=scratch,
        name="pack",
    )(place, *operands)


def stage_body(_, out):
    out[...] = jnp.zeros(out.shape, out.dtype)


def stage(value):
    return pl.pallas_call(
        stage_body,
        out_shape=jax.ShapeDtypeStruct((8, HD), jnp.float32),
        in_specs=[VMEM],
        out_specs=VMEM,
        compiler_params=pltpu.CompilerParams(vmem_limit_bytes=VMEM_LIMIT),
        name="stage",
    )(value)


def attention_body(
    place, bias_ref, *rest, rows, half, heads, low, inner, outer, group, partial, held
):
    kv_rows = 2 * half + 2 * rows
    refs, rest = rest[:group], rest[group:]
    own = [(ref, 0, low if step < inner else 0) for step, ref in enumerate(refs)]
    other = [(rest[0], step * kv_rows, low) for step in range(inner)]
    rest = rest[1:]
    if inner < group:
        other += [(rest[0], step * kv_rows, 0) for step in range(group - inner)]
        rest = rest[1:]
    q_all = None
    if partial:
        q_all, rest = rest[0], rest[1:]
    rest = rest[held:]
    out_ref, stats, q_scr = rest[0], rest[1:-1], rest[-1]
    singles = () if partial else stats
    for step, (ref, _, base) in enumerate(own):
        member = place[0] ^ step
        for o in range(outer):
            at = pl.multiple_of((o * group + member) * rows, 8)
            if partial:
                q_scr[pl.ds(at, rows), :] = q_all[o, step]
            else:
                q_scr[pl.ds(at, rows), :] = ref[kv_rows:, base : base + heads * HD]
    total_rows = outer * group * rows
    block_count = bias_ref.shape[0]
    q_block = total_rows // block_count

    for h in range(heads):
        cols = slice(h * HD, (h + 1) * HD)
        queries = q_scr[:, cols]

        def flat(sources, first, count):
            pieces = []
            for ref, row, base in sources:
                columns = slice(base + h * HD, base + (h + 1) * HD)
                pieces.append(ref[row + first : row + first + count, columns])
            return jnp.concatenate(pieces, axis=0)

        peak = total = acc = None
        column = 0
        for sources, first, count, value_first in (
            (own, 2 * half, rows, 2 * half + rows),
            (other, 2 * half, rows, 2 * half + rows),
            (own, 0, half, half),
            (other, 0, half, half),
        ):
            keys = flat(sources, first, count)
            values = flat(sources, value_first, count)
            width = keys.shape[0]
            scores = lax.dot_general(
                queries, keys, (((1,), (1,)), ((), ())), preferred_element_type=jnp.float32
            )
            scores = scores.reshape(block_count, q_block, width) * LOG2_SCALE
            scores = scores + bias_ref[:, :, column : column + width]
            scores = scores.reshape(total_rows, width)
            column += width
            top = jnp.max(scores, axis=1, keepdims=True)
            new_peak = top if peak is None else jnp.maximum(peak, top)
            weights = jnp.exp2(scores - new_peak)
            part = jnp.sum(weights, axis=1, keepdims=True)
            product = jnp.dot(
                weights.astype(jnp.bfloat16), values, preferred_element_type=jnp.float32
            )
            if peak is None:
                total, acc = part, product
            else:
                scale = jnp.exp2(peak - new_peak)
                total = total * scale + part
                acc = acc * scale + product
            peak = new_peak
        if partial:
            out_ref[:, cols] = acc
            stats[0][:, h : h + 1] = peak
            stats[1][:, h : h + 1] = total
        else:
            result = (acc / total).astype(out_ref.dtype)
            out_ref[:, cols] = result
            if singles:
                singles[h][...] = result


def attention(place, bias, own, others, q_all, held, rows, half, total_rows, low, cols):
    group = len(own)
    partial = q_all is not None
    wide = jax.ShapeDtypeStruct((total_rows, cols), jnp.float32 if partial else jnp.bfloat16)
    thin = jax.ShapeDtypeStruct((total_rows, cols // HD), jnp.float32)
    body = functools.partial(
        attention_body,
        rows=rows,
        half=half,
        heads=cols // HD,
        low=low,
        inner=max(group // 2, 1),
        outer=total_rows // (group * rows),
        group=group,
        partial=partial,
        held=len(held),
    )
    operands = (*own, *others) + ((q_all,) if partial else ()) + held
    single = jax.ShapeDtypeStruct((total_rows, HD), jnp.bfloat16)
    heads = cols // HD
    outs = (wide, thin, thin) if partial else (wide,) + (single,) * (heads if heads > 1 else 0)
    return pl.pallas_call(
        body,
        out_shape=outs,
        in_specs=[SMEM] + [VMEM] * (1 + len(operands)),
        out_specs=(VMEM,) * len(outs),
        scratch_shapes=[pltpu.VMEM((total_rows, cols), jnp.bfloat16)],
        compiler_params=pltpu.CompilerParams(vmem_limit_bytes=VMEM_LIMIT),
        name="attend",
    )(place, bias, *operands)


def project_body(place, weight, *rest, rows, last, first):
    count = len(rows)
    parts, rest = rest[:count], rest[count:]
    left = jnp.concatenate([part[...] for part in parts], axis=1)
    right = jnp.concatenate(
        [
            weight[pl.ds(pl.multiple_of((place[0] ^ step) * width + low, HD), part.shape[1]), :]
            for part, (step, low, width) in zip(parts, rows)
        ],
        axis=0,
    )
    acc = jnp.dot(left, right, preferred_element_type=jnp.float32)
    if not first:
        acc = acc + rest[0][...]
        rest = rest[1:]
    if last:
        gate, out = rest
        acc = acc * gate[pl.ds(place[2] % 8, 1), :]
    else:
        (out,) = rest
    out[...] = acc.astype(out.dtype)


def project(place, entries, weight, before, gate, width):
    parts = [part for part, _, _ in entries]
    rows = tuple((step, low, width) for _, step, low in entries)
    first, last = before is None, gate is not None
    operands = [weight, *parts]
    operands += [] if first else [before]
    operands += [gate] if last else []
    shape = (parts[0].shape[0], weight.shape[1])
    return pl.pallas_call(
        functools.partial(project_body, rows=rows, last=last, first=first),
        out_shape=jax.ShapeDtypeStruct(shape, jnp.bfloat16 if last else jnp.float32),
        in_specs=[SMEM] + [VMEM] * len(operands),
        out_specs=VMEM,
        compiler_params=pltpu.CompilerParams(vmem_limit_bytes=VMEM_LIMIT),
        name="project",
    )(place, *operands)


def bias_body(place, mask, out, *, group, rows, half, history_rows):
    block_count = out.shape[0]
    fresh, history = group * rows, group * half
    member, core, base, live_limit = place[0], place[1], place[3], place[4]

    def positions(count, size, offset):
        column = lax.broadcasted_iota(jnp.int32, (1, count * group), 1)
        position = column
        for step in range(group):
            start = (base + (member ^ step)) * size + offset - step * count
            position = jnp.where(column >= step * count, column + start, position)
        return position

    def put(row, low, allowed):
        out[row, :, low : low + allowed.shape[1]] = jnp.where(allowed > 0, 0.0, NEGATIVE)

    position = positions(rows, rows, 0)
    for row in range(block_count):
        for low, first in ((0, block_count), (fresh, 0)):
            allowed = jnp.zeros(position.shape, jnp.int32)
            for block in range(block_count):
                within = (position >= block * BLK) & (position < (block + 1) * BLK)
                allowed = jnp.where(within, mask[row, first + block], allowed)
            put(row, low, allowed)
    for low, which in ((2 * fresh, core), (2 * fresh + history, 1 - core)):
        position = positions(half, history_rows, which * half)
        allowed = jnp.where(position < live_limit, 1, 0)
        for row in range(block_count):
            put(row, low, allowed)


def key_bias(place, block_mask, group, rows, half, history_rows):
    keys = 2 * group * (rows + half)
    return pl.pallas_call(
        functools.partial(
            bias_body, group=group, rows=rows, half=half, history_rows=history_rows
        ),
        out_shape=jax.ShapeDtypeStruct((block_mask.shape[0], 1, keys), jnp.float32),
        in_specs=[SMEM, SMEM],
        out_specs=VMEM,
        compiler_params=pltpu.CompilerParams(vmem_limit_bytes=VMEM_LIMIT),
        name="bias",
    )(place, block_mask)


def on_device(
    query, stretch_kv, history_kv, block_mask, noise_level, history_blocks, out_weight, gate_table
):
    tp_count = lax.axis_size("tp")
    tp_index = lax.axis_index("tp")
    core = lax.axis_index("stretch")
    rows = query.shape[1]
    feature_width = query.shape[2]
    history_rows = history_kv.shape[1]
    half = history_rows // 2
    group = head_groups(feature_width // HD, tp_count)
    outer = tp_count // group
    width = feature_width // group
    total_rows = tp_count * rows
    member = tp_index % group
    kv_rows = 2 * half + 2 * rows
    place = [member, core, noise_level[0], tp_index - member, history_blocks[0] * BLK]
    place = jnp.stack(place).astype(jnp.int32)
    same = [[o * group + m for o in range(outer)] for m in range(group)]
    chunks = [(low * HD, count * HD) for low, count in head_chunks(width // HD, CHUNKS)]

    bias = key_bias(place, block_mask[0], group, rows, half, history_rows)

    inner = max(group // 2, 1)
    cross = list(range(group - 1, inner - 1, -1))
    arrays = (query[0], stretch_kv[:, 0], history_kv)
    plan = [(step, low, cols) for low, cols in chunks[:1] for step in cross]
    blocks = pack(place, *arrays, width, plan) if plan else ()
    rest = [(step, 0, width) for step in range(inner)]
    rest += [(step, low, cols) for low, cols in chunks[1:] for step in cross]
    gate_rows, *others = pack(place, *arrays, width, rest, gate_table)
    blocks = list(blocks) + others
    plan += rest
    sends = [{} for _ in chunks]
    near = {}
    for (step, low, cols), block in zip(plan, blocks):
        if step >= inner:
            index = [first for first, _ in chunks].index(low)
            sends[index][step] = xor_permute(block, group, step)
        elif step == 0:
            near[step] = block
        else:
            near[step] = xor_permute(block, group, step)
    other_near = partner_core(
        jnp.concatenate([near[step][:kv_rows] for step in range(inner)], axis=0)
    )

    held = (out_weight, stage(out_weight))
    groups = [[] for _ in range(len(chunks) + 1)]
    for index, (low, cols) in enumerate(chunks):
        far = sends[index]
        own = [near[step] for step in range(inner)] + [far[step] for step in reversed(cross)]
        others = [other_near]
        if cross:
            others.append(
                partner_core(
                    jnp.concatenate([far[step][:kv_rows] for step in reversed(cross)], axis=0)
                )
            )
        attend = functools.partial(
            attention,
            place,
            bias,
            own,
            others,
            held=held,
            rows=rows,
            half=half,
            total_rows=total_rows,
            low=low,
            cols=cols,
        )
        if outer > 1:
            q = jnp.stack(
                [
                    block[kv_rows:, low : low + cols] if step < inner else block[kv_rows:]
                    for step, block in enumerate(own)
                ]
            )
            q = lax.all_gather(q, "tp", axis=0, axis_index_groups=same)
            out, peak, total = attend(q_all=q)
            outs, peaks, totals = (
                lax.all_gather(value, "tp", axis=0, axis_index_groups=same)
                for value in (out, peak, total)
            )
            factor = jnp.exp2(peaks - jnp.max(peaks, axis=0, keepdims=True))
            total = jnp.sum(totals * factor, axis=0)
            outs = outs.reshape(outer, total_rows, -1, HD) * factor[..., None]
            attended = (jnp.sum(outs, axis=0) / total[..., None]).astype(jnp.bfloat16)
            attended = attended.reshape(total_rows, -1)
            singles = [attended[:, at : at + HD] for at in range(0, cols, HD)]
        else:
            attended, *singles = attend(q_all=None)
            singles = singles or [attended]
        close, distant = spread(attended, singles, group)
        groups[index] += [(value, step, low) for value, step in close]
        for head, pieces in enumerate(distant):
            late = min(index + (1 if head < len(distant) - 1 else 2), len(chunks))
            groups[late] += [(value, step, low + head * HD) for value, step in pieces]

    groups = [entries for entries in groups if entries]
    result = None
    for index, entries in enumerate(groups):
        gate = gate_rows if index == len(groups) - 1 else None
        result = project(place, entries, out_weight, result, gate, width)
    return result[None]


def solution(mesh):
    return jax.shard_map(
        on_device,
        mesh=mesh,
        in_specs=(
            P(("rep", "stretch"), "tp", None),
            P(None, ("rep", "stretch"), "tp", None),
            P(None, ("rep", "tp"), None),
            P(("rep", "stretch"), None, None),
            P(("rep", "stretch")),
            P("rep"),
            P(None, "tp"),
            P(None, "tp"),
        ),
        out_specs=P(("rep", "stretch"), None, "tp"),
        check_vma=False,
    )
```

```python
import functools
import math

import jax
import jax.numpy as jnp
from jax import lax
from jax.experimental import pallas as pl
from jax.experimental.pallas import tpu as pltpu
from jax.sharding import PartitionSpec as P


HD = 128
BLK = 128
NEGATIVE = -1e30
LOG2_SCALE = math.log2(math.e) / math.sqrt(HD)
CHUNKS = 2
VMEM_LIMIT = 12 << 20

VMEM = pl.BlockSpec(memory_space=pltpu.VMEM)
SMEM = pl.BlockSpec(memory_space=pltpu.SMEM)
HBM = pl.BlockSpec(memory_space=pltpu.HBM)


def head_groups(head_count, tp_count):
    both = math.gcd(head_count, tp_count)
    return both & -both


def head_chunks(heads, count):
    count = min(count, heads)
    sizes = [heads // count + (1 if i < heads % count else 0) for i in range(count)]
    return [(sum(sizes[:i]), sizes[i]) for i in range(count)]


def xor_permute(value, group, step, senders=None):
    count = lax.axis_size("tp")
    pairs = [
        (t, (t // group) * group + ((t % group) ^ step))
        for t in range(count)
        if senders is None or t % group in senders
    ]
    return lax.ppermute(value, "tp", pairs)


def spread(value, heads, group, across_first):
    def send(block, step):
        return xor_permute(block, group, step)

    def both(block, step):
        return [(block, step), (send(block, 1), step ^ 1)]

    if group == 1:
        return [(value, 0)], [[] for _ in heads]
    near = both(value, 0)
    if group == 8:
        pair = send(value, 2)
        if across_first:
            near += [(pair, 2), (send(near[1][0], 2), 3)]
        else:
            near += both(pair, 2)
    far = []
    for head, block in enumerate(heads):
        pieces = []
        if group == 8:
            over = send(block, 4)
            if across_first:
                crossed = near[1][0][:, head * HD : (head + 1) * HD]
                crossed_over = send(crossed, 4)
                pieces += [(over, 4), (crossed_over, 5)]
                pieces += [(send(over, 2), 6)]
                pieces += [(send(crossed_over, 2), 7)]
            else:
                pieces += both(over, 4)
                pieces += both(send(over, 2), 6)
        else:
            for step in range(2, group, 2):
                moved = send(block, step)
                pieces += both(moved, step)
        far.append(pieces)
    return near, far


def partner_core(value):
    return lax.ppermute(value, "stretch", [(0, 1), (1, 0)])


def pack_body(*rest, half, rows, width, plan, gated, group):
    member, core = lax.axis_index("tp") % group, lax.axis_index("stretch")
    if gated:
        place, table, rest = rest[0], rest[1], rest[2:]
    query, stretch, history, rest = *rest[:3], rest[3:]
    count = len(plan)
    if gated:
        gate_out, rest = rest[0], rest[1:]
        gate_sem, rest = rest[-1], rest[:-1]
        gate_row = pl.multiple_of(place[2] // 8 * 8, 8)
        gate_copy = pltpu.make_async_copy(table.at[pl.ds(gate_row, 8), :], gate_out, gate_sem)
        gate_copy.start()
    blocks, stages = rest[:count], rest[count : 2 * count]
    in_sems, out_sems = rest[2 * count :]
    row = pl.multiple_of(core * half, 8)
    incoming = []
    for index, (step, low, cols) in enumerate(plan):
        column = pl.ds(pl.multiple_of((member ^ step) * width + low, HD), cols)
        parts = (
            (history.at[0, pl.ds(row, half), column], 0, half),
            (history.at[1, pl.ds(row, half), column], half, half),
            (stretch.at[0, :, column], 2 * half, rows),
            (stretch.at[1, :, column], 2 * half + rows, rows),
            (query.at[:, column], 2 * half + 2 * rows, rows),
        )
        copies = [
            pltpu.make_async_copy(
                source, stages[index].at[pl.ds(at, size), :], in_sems.at[index, part]
            )
            for part, (source, at, size) in enumerate(parts)
        ]
        for copy in copies:
            copy.start()
        incoming.append(copies)
    outgoing = []
    for index, copies in enumerate(incoming):
        for copy in copies:
            copy.wait()
        copy = pltpu.make_async_copy(stages[index], blocks[index], out_sems.at[index])
        copy.start()
        outgoing.append(copy)
    for copy in outgoing:
        copy.wait()
    if gated:
        gate_copy.wait()


def pack(query, stretch, history, width, plan, group, place=None, table=None):
    gated = table is not None
    rows, half = query.shape[0], history.shape[1] // 2
    shapes = [(2 * half + 3 * rows, cols) for _, _, cols in plan]
    outs = [jax.ShapeDtypeStruct(shape, query.dtype) for shape in shapes]
    scratch = [pltpu.VMEM(shape, query.dtype) for shape in shapes]
    scratch += [pltpu.SemaphoreType.DMA((len(plan), 5)), pltpu.SemaphoreType.DMA((len(plan),))]
    operands = [query, stretch, history]
    out_specs = [HBM] * len(plan)
    if gated:
        outs = [jax.ShapeDtypeStruct((8, table.shape[1]), table.dtype)] + outs
        out_specs = [VMEM] + out_specs
        scratch.append(pltpu.SemaphoreType.DMA)
        operands = [place, table] + operands
    return pl.pallas_call(
        functools.partial(
            pack_body, half=half, rows=rows, width=width, plan=plan, gated=gated, group=group
        ),
        out_shape=tuple(outs),
        in_specs=([SMEM, HBM] if gated else []) + [HBM] * 3,
        out_specs=tuple(out_specs),
        scratch_shapes=scratch,
        name="pack",
    )(*operands)


def stage_body(_, out):
    out[...] = jnp.zeros(out.shape, out.dtype)


def stage(value):
    return pl.pallas_call(
        stage_body,
        out_shape=jax.ShapeDtypeStruct((8, HD), jnp.float32),
        in_specs=[VMEM],
        out_specs=VMEM,
        compiler_params=pltpu.CompilerParams(vmem_limit_bytes=VMEM_LIMIT),
        name="stage",
    )(value)


def attention_body(
    place, bias_ref, *rest, rows, half, heads, low, inner, outer, group, partial, held
):
    kv_rows = 2 * half + 2 * rows
    refs, rest = rest[:group], rest[group:]
    own = [(ref, 0, low if step < inner else 0) for step, ref in enumerate(refs)]
    other = [(rest[0], step * kv_rows, low) for step in range(inner)]
    rest = rest[1:]
    if inner < group:
        other += [(rest[0], step * kv_rows, 0) for step in range(group - inner)]
        rest = rest[1:]
    q_all = None
    if partial:
        q_all, rest = rest[0], rest[1:]
    rest = rest[held:]
    out_ref, stats, q_scr = rest[0], rest[1:-1], rest[-1]
    singles = () if partial else stats
    for step, (ref, _, base) in enumerate(own):
        member = place[0] ^ step
        for o in range(outer):
            at = pl.multiple_of((o * group + member) * rows, 8)
            if partial:
                q_scr[pl.ds(at, rows), :] = q_all[o, step]
            else:
                q_scr[pl.ds(at, rows), :] = ref[kv_rows:, base : base + heads * HD]
    total_rows = outer * group * rows
    block_count = bias_ref.shape[0]
    q_block = total_rows // block_count

    for h in range(heads):
        cols = slice(h * HD, (h + 1) * HD)
        queries = q_scr[:, cols]

        def flat(sources, first, count):
            pieces = []
            for ref, row, base in sources:
                columns = slice(base + h * HD, base + (h + 1) * HD)
                pieces.append(ref[row + first : row + first + count, columns])
            return jnp.concatenate(pieces, axis=0)

        peak = total = acc = None
        column = 0
        for sources, first, count, value_first in (
            (own, 2 * half, rows, 2 * half + rows),
            (other, 2 * half, rows, 2 * half + rows),
            (own, 0, half, half),
            (other, 0, half, half),
        ):
            keys = flat(sources, first, count)
            values = flat(sources, value_first, count)
            width = keys.shape[0]
            scores = lax.dot_general(
                queries, keys, (((1,), (1,)), ((), ())), preferred_element_type=jnp.float32
            )
            scores = scores.reshape(block_count, q_block, width) * LOG2_SCALE
            scores = scores + bias_ref[:, :, column : column + width]
            scores = scores.reshape(total_rows, width)
            column += width
            top = jnp.max(scores, axis=1, keepdims=True)
            new_peak = top if peak is None else jnp.maximum(peak, top)
            weights = jnp.exp2(scores - new_peak)
            part = jnp.sum(weights, axis=1, keepdims=True)
            product = jnp.dot(
                weights.astype(jnp.bfloat16), values, preferred_element_type=jnp.float32
            )
            if peak is None:
                total, acc = part, product
            else:
                scale = jnp.exp2(peak - new_peak)
                total = total * scale + part
                acc = acc * scale + product
            peak = new_peak
        if partial:
            out_ref[:, cols] = acc
            stats[0][:, h : h + 1] = peak
            stats[1][:, h : h + 1] = total
        else:
            result = (acc / total).astype(out_ref.dtype)
            out_ref[:, cols] = result
            if singles:
                singles[h][...] = result


def attention(place, bias, own, others, q_all, held, rows, half, total_rows, low, cols):
    group = len(own)
    partial = q_all is not None
    wide = jax.ShapeDtypeStruct((total_rows, cols), jnp.float32 if partial else jnp.bfloat16)
    thin = jax.ShapeDtypeStruct((total_rows, cols // HD), jnp.float32)
    body = functools.partial(
        attention_body,
        rows=rows,
        half=half,
        heads=cols // HD,
        low=low,
        inner=max(group // 2, 1),
        outer=total_rows // (group * rows),
        group=group,
        partial=partial,
        held=len(held),
    )
    operands = (*own, *others) + ((q_all,) if partial else ()) + held
    single = jax.ShapeDtypeStruct((total_rows, HD), jnp.bfloat16)
    heads = cols // HD
    outs = (wide, thin, thin) if partial else (wide,) + (single,) * (heads if heads > 1 else 0)
    return pl.pallas_call(
        body,
        out_shape=outs,
        in_specs=[SMEM] + [VMEM] * (1 + len(operands)),
        out_specs=(VMEM,) * len(outs),
        scratch_shapes=[pltpu.VMEM((total_rows, cols), jnp.bfloat16)],
        compiler_params=pltpu.CompilerParams(vmem_limit_bytes=VMEM_LIMIT),
        name="attend",
    )(place, bias, *operands)


def project_body(place, weight, *rest, rows, last, first):
    count = len(rows)
    parts, rest = rest[:count], rest[count:]
    left = jnp.concatenate([part[...] for part in parts], axis=1)
    right = jnp.concatenate(
        [
            weight[pl.ds(pl.multiple_of((place[0] ^ step) * width + low, HD), part.shape[1]), :]
            for part, (step, low, width) in zip(parts, rows)
        ],
        axis=0,
    )
    acc = jnp.dot(left, right, preferred_element_type=jnp.float32)
    if not first:
        acc = acc + rest[0][...]
        rest = rest[1:]
    if last:
        gate, out = rest
        acc = acc * gate[pl.ds(place[2] % 8, 1), :]
    else:
        (out,) = rest
    out[...] = acc.astype(out.dtype)


def project(place, entries, weight, before, gate, width):
    parts = [part for part, _, _ in entries]
    rows = tuple((step, low, width) for _, step, low in entries)
    first, last = before is None, gate is not None
    operands = [weight, *parts]
    operands += [] if first else [before]
    operands += [gate] if last else []
    shape = (parts[0].shape[0], weight.shape[1])
    return pl.pallas_call(
        functools.partial(project_body, rows=rows, last=last, first=first),
        out_shape=jax.ShapeDtypeStruct(shape, jnp.bfloat16 if last else jnp.float32),
        in_specs=[SMEM] + [VMEM] * len(operands),
        out_specs=VMEM,
        compiler_params=pltpu.CompilerParams(vmem_limit_bytes=VMEM_LIMIT),
        name="project",
    )(place, *operands)


def bias_body(place, mask, out, *, group, rows, half, history_rows):
    block_count = out.shape[0]
    fresh, history = group * rows, group * half
    member, core, base, live_limit = place[0], place[1], place[3], place[4]

    def positions(count, size, offset):
        column = lax.broadcasted_iota(jnp.int32, (1, count * group), 1)
        position = column
        for step in range(group):
            start = (base + (member ^ step)) * size + offset - step * count
            position = jnp.where(column >= step * count, column + start, position)
        return position

    def put(row, low, allowed):
        out[row, :, low : low + allowed.shape[1]] = jnp.where(allowed > 0, 0.0, NEGATIVE)

    position = positions(rows, rows, 0)
    for row in range(block_count):
        for low, first in ((0, block_count), (fresh, 0)):
            allowed = jnp.zeros(position.shape, jnp.int32)
            for block in range(block_count):
                within = (position >= block * BLK) & (position < (block + 1) * BLK)
                allowed = jnp.where(within, mask[row, first + block], allowed)
            put(row, low, allowed)
    for low, which in ((2 * fresh, core), (2 * fresh + history, 1 - core)):
        position = positions(half, history_rows, which * half)
        allowed = jnp.where(position < live_limit, 1, 0)
        for row in range(block_count):
            put(row, low, allowed)


def key_bias(place, block_mask, group, rows, half, history_rows):
    keys = 2 * group * (rows + half)
    return pl.pallas_call(
        functools.partial(
            bias_body, group=group, rows=rows, half=half, history_rows=history_rows
        ),
        out_shape=jax.ShapeDtypeStruct((block_mask.shape[0], 1, keys), jnp.float32),
        in_specs=[SMEM, SMEM],
        out_specs=VMEM,
        compiler_params=pltpu.CompilerParams(vmem_limit_bytes=VMEM_LIMIT),
        name="bias",
    )(place, block_mask)


def on_device(
    query, stretch_kv, history_kv, block_mask, noise_level, history_blocks, out_weight, gate_table
):
    tp_count = lax.axis_size("tp")
    tp_index = lax.axis_index("tp")
    core = lax.axis_index("stretch")
    rows = query.shape[1]
    feature_width = query.shape[2]
    history_rows = history_kv.shape[1]
    half = history_rows // 2
    group = head_groups(feature_width // HD, tp_count)
    outer = tp_count // group
    width = feature_width // group
    total_rows = tp_count * rows
    member = tp_index % group
    kv_rows = 2 * half + 2 * rows
    place = [member, core, noise_level[0], tp_index - member, history_blocks[0] * BLK]
    place = jnp.stack(place).astype(jnp.int32)
    same = [[o * group + m for o in range(outer)] for m in range(group)]
    chunks = [(low * HD, count * HD) for low, count in head_chunks(width // HD, CHUNKS)]

    bias = key_bias(place, block_mask[0], group, rows, half, history_rows)

    inner = max(group // 2, 1)
    cross = list(range(group - 1, inner - 1, -1))
    arrays = (query[0], stretch_kv[:, 0], history_kv)
    plan = [(step, low, cols) for low, cols in chunks[:1] for step in cross]
    blocks = pack(*arrays, width, plan, group) if plan else ()
    rest = [(step, 0, width) for step in range(inner)]
    rest += [(step, low, cols) for low, cols in chunks[1:] for step in cross]
    gate_rows, *others = pack(*arrays, width, rest, group, place, gate_table)
    blocks = list(blocks) + others
    plan += rest
    sends = [{} for _ in chunks]
    near = {}
    for (step, low, cols), block in zip(plan, blocks):
        if step >= inner:
            index = [first for first, _ in chunks].index(low)
            sends[index][step] = xor_permute(block, group, step)
        elif step == 0:
            near[step] = block
        else:
            near[step] = xor_permute(block, group, step)
    other_near = partner_core(
        jnp.concatenate([near[step][:kv_rows] for step in range(inner)], axis=0)
    )

    held = (out_weight, stage(out_weight))
    groups = [[] for _ in range(len(chunks) + 1)]
    for index, (low, cols) in enumerate(chunks):
        far = sends[index]
        own = [near[step] for step in range(inner)] + [far[step] for step in reversed(cross)]
        others = [other_near]
        if cross:
            others.append(
                partner_core(
                    jnp.concatenate([far[step][:kv_rows] for step in reversed(cross)], axis=0)
                )
            )
        attend = functools.partial(
            attention,
            place,
            bias,
            own,
            others,
            held=held,
            rows=rows,
            half=half,
            total_rows=total_rows,
            low=low,
            cols=cols,
        )
        if outer > 1:
            q = jnp.stack(
                [
                    block[kv_rows:, low : low + cols] if step < inner else block[kv_rows:]
                    for step, block in enumerate(own)
                ]
            )
            q = lax.all_gather(q, "tp", axis=0, axis_index_groups=same)
            out, peak, total = attend(q_all=q)
            outs, peaks, totals = (
                lax.all_gather(value, "tp", axis=0, axis_index_groups=same)
                for value in (out, peak, total)
            )
            factor = jnp.exp2(peaks - jnp.max(peaks, axis=0, keepdims=True))
            total = jnp.sum(totals * factor, axis=0)
            outs = outs.reshape(outer, total_rows, -1, HD) * factor[..., None]
            attended = (jnp.sum(outs, axis=0) / total[..., None]).astype(jnp.bfloat16)
            attended = attended.reshape(total_rows, -1)
            singles = [attended[:, at : at + HD] for at in range(0, cols, HD)]
        else:
            attended, *singles = attend(q_all=None)
            singles = singles or [attended]
        close, distant = spread(attended, singles, group, index == len(chunks) - 1)
        groups[index] += [(value, step, low) for value, step in close]
        for head, pieces in enumerate(distant):
            late = min(index + (1 if head < len(distant) - 1 else 2), len(chunks))
            groups[late] += [(value, step, low + head * HD) for value, step in pieces]

    groups = [entries for entries in groups if entries]
    result = None
    for index, entries in enumerate(groups):
        gate = gate_rows if index == len(groups) - 1 else None
        result = project(place, entries, out_weight, result, gate, width)
    return result[None]


def solution(mesh):
    return jax.shard_map(
        on_device,
        mesh=mesh,
        in_specs=(
            P(("rep", "stretch"), "tp", None),
            P(None, ("rep", "stretch"), "tp", None),
            P(None, ("rep", "tp"), None),
            P(("rep", "stretch"), None, None),
            P(("rep", "stretch")),
            P("rep"),
            P(None, "tp"),
            P(None, "tp"),
        ),
        out_specs=P(("rep", "stretch"), None, "tp"),
        check_vma=False,
    )
```

```python
import functools
import math

import jax
import jax.numpy as jnp
from jax import lax
from jax.experimental import pallas as pl
from jax.experimental.pallas import tpu as pltpu
from jax.sharding import PartitionSpec as P


HD = 128
BLK = 128
NEGATIVE = -1e30
LOG2_SCALE = math.log2(math.e) / math.sqrt(HD)
CHUNKS = 2
VMEM_LIMIT = 12 << 20

VMEM = pl.BlockSpec(memory_space=pltpu.VMEM)
SMEM = pl.BlockSpec(memory_space=pltpu.SMEM)
HBM = pl.BlockSpec(memory_space=pltpu.HBM)


def head_groups(head_count, tp_count):
    both = math.gcd(head_count, tp_count)
    return both & -both


def head_chunks(heads, count):
    count = min(count, heads)
    sizes = [heads // count + (1 if i < heads % count else 0) for i in range(count)]
    return [(sum(sizes[:i]), sizes[i]) for i in range(count)]


def xor_permute(value, group, step, senders=None):
    count = lax.axis_size("tp")
    pairs = [
        (t, (t // group) * group + ((t % group) ^ step))
        for t in range(count)
        if senders is None or t % group in senders
    ]
    return lax.ppermute(value, "tp", pairs)


def spread(value, heads, group, across_first):
    def send(block, step):
        return xor_permute(block, group, step)

    def both(block, step):
        return [(block, step), (send(block, 1), step ^ 1)]

    if group == 1:
        return [(value, 0)], [[] for _ in heads]
    near = both(value, 0)
    if group == 8:
        near += both(send(value, 2), 2)
    far = []
    for head, block in enumerate(heads):
        pieces = []
        if group == 8:
            over = send(block, 4)
            if across_first:
                crossed = near[1][0][:, head * HD : (head + 1) * HD]
                crossed_over = send(crossed, 4)
                pieces += [(over, 4), (crossed_over, 5)]
                pieces += [(send(over, 2), 6)]
                pieces += [(send(crossed_over, 2), 7)]
            else:
                pieces += both(over, 4)
                pieces += both(send(over, 2), 6)
        else:
            for step in range(2, group, 2):
                moved = send(block, step)
                pieces += both(moved, step)
        far.append(pieces)
    return near, far


def partner_core(value):
    return lax.ppermute(value, "stretch", [(0, 1), (1, 0)])


def pack_body(*rest, half, rows, width, plan, gated, group):
    member, core = lax.axis_index("tp") % group, lax.axis_index("stretch")
    if gated:
        place, table, rest = rest[0], rest[1], rest[2:]
    query, stretch, history, rest = *rest[:3], rest[3:]
    count = len(plan)
    if gated:
        gate_out, rest = rest[0], rest[1:]
        gate_sem, rest = rest[-1], rest[:-1]
        gate_row = pl.multiple_of(place[2] // 8 * 8, 8)
        gate_copy = pltpu.make_async_copy(table.at[pl.ds(gate_row, 8), :], gate_out, gate_sem)
        gate_copy.start()
    blocks, stages = rest[:count], rest[count : 2 * count]
    in_sems, out_sems = rest[2 * count :]
    row = pl.multiple_of(core * half, 8)
    incoming = []
    for index, (step, low, cols) in enumerate(plan):
        column = pl.ds(pl.multiple_of((member ^ step) * width + low, HD), cols)
        parts = (
            (history.at[0, pl.ds(row, half), column], 0, half),
            (history.at[1, pl.ds(row, half), column], half, half),
            (stretch.at[0, :, column], 2 * half, rows),
            (stretch.at[1, :, column], 2 * half + rows, rows),
            (query.at[:, column], 2 * half + 2 * rows, rows),
        )
        copies = [
            pltpu.make_async_copy(
                source, stages[index].at[pl.ds(at, size), :], in_sems.at[index, part]
            )
            for part, (source, at, size) in enumerate(parts)
        ]
        for copy in copies:
            copy.start()
        incoming.append(copies)
    outgoing = []
    for index, copies in enumerate(incoming):
        for copy in copies:
            copy.wait()
        copy = pltpu.make_async_copy(stages[index], blocks[index], out_sems.at[index])
        copy.start()
        outgoing.append(copy)
    for copy in outgoing:
        copy.wait()
    if gated:
        gate_copy.wait()


def pack(query, stretch, history, width, plan, group, place=None, table=None):
    gated = table is not None
    rows, half = query.shape[0], history.shape[1] // 2
    shapes = [(2 * half + 3 * rows, cols) for _, _, cols in plan]
    outs = [jax.ShapeDtypeStruct(shape, query.dtype) for shape in shapes]
    scratch = [pltpu.VMEM(shape, query.dtype) for shape in shapes]
    scratch += [pltpu.SemaphoreType.DMA((len(plan), 5)), pltpu.SemaphoreType.DMA((len(plan),))]
    operands = [query, stretch, history]
    out_specs = [HBM] * len(plan)
    if gated:
        outs = [jax.ShapeDtypeStruct((8, table.shape[1]), table.dtype)] + outs
        out_specs = [VMEM] + out_specs
        scratch.append(pltpu.SemaphoreType.DMA)
        operands = [place, table] + operands
    return pl.pallas_call(
        functools.partial(
            pack_body, half=half, rows=rows, width=width, plan=plan, gated=gated, group=group
        ),
        out_shape=tuple(outs),
        in_specs=([SMEM, HBM] if gated else []) + [HBM] * 3,
        out_specs=tuple(out_specs),
        scratch_shapes=scratch,
        name="pack",
    )(*operands)


def stage_body(_, out):
    out[...] = jnp.zeros(out.shape, out.dtype)


def stage(value):
    return pl.pallas_call(
        stage_body,
        out_shape=jax.ShapeDtypeStruct((8, HD), jnp.float32),
        in_specs=[VMEM],
        out_specs=VMEM,
        compiler_params=pltpu.CompilerParams(vmem_limit_bytes=VMEM_LIMIT),
        name="stage",
    )(value)


def attention_body(
    place, bias_ref, *rest, rows, half, heads, low, inner, outer, group, partial, held
):
    kv_rows = 2 * half + 2 * rows
    refs, rest = rest[:group], rest[group:]
    own = [(ref, 0, low if step < inner else 0) for step, ref in enumerate(refs)]
    other = [(rest[0], step * kv_rows, low) for step in range(inner)]
    rest = rest[1:]
    if inner < group:
        other += [(rest[0], step * kv_rows, 0) for step in range(group - inner)]
        rest = rest[1:]
    q_all = None
    if partial:
        q_all, rest = rest[0], rest[1:]
    rest = rest[held:]
    out_ref, stats, q_scr = rest[0], rest[1:-1], rest[-1]
    singles = () if partial else stats
    for step, (ref, _, base) in enumerate(own):
        member = place[0] ^ step
        for o in range(outer):
            at = pl.multiple_of((o * group + member) * rows, 8)
            if partial:
                q_scr[pl.ds(at, rows), :] = q_all[o, step]
            else:
                q_scr[pl.ds(at, rows), :] = ref[kv_rows:, base : base + heads * HD]
    total_rows = outer * group * rows
    block_count = bias_ref.shape[0]
    q_block = total_rows // block_count

    for h in range(heads):
        cols = slice(h * HD, (h + 1) * HD)
        queries = q_scr[:, cols]

        def flat(sources, first, count):
            pieces = []
            for ref, row, base in sources:
                columns = slice(base + h * HD, base + (h + 1) * HD)
                pieces.append(ref[row + first : row + first + count, columns])
            return jnp.concatenate(pieces, axis=0)

        peak = total = acc = None
        column = 0
        for sources, first, count, value_first in (
            (own, 2 * half, rows, 2 * half + rows),
            (other, 2 * half, rows, 2 * half + rows),
            (own, 0, half, half),
            (other, 0, half, half),
        ):
            keys = flat(sources, first, count)
            values = flat(sources, value_first, count)
            width = keys.shape[0]
            scores = lax.dot_general(
                queries, keys, (((1,), (1,)), ((), ())), preferred_element_type=jnp.float32
            )
            scores = scores.reshape(block_count, q_block, width) * LOG2_SCALE
            scores = scores + bias_ref[:, :, column : column + width]
            scores = scores.reshape(total_rows, width)
            column += width
            top = jnp.max(scores, axis=1, keepdims=True)
            new_peak = top if peak is None else jnp.maximum(peak, top)
            weights = jnp.exp2(scores - new_peak)
            part = jnp.sum(weights, axis=1, keepdims=True)
            product = jnp.dot(
                weights.astype(jnp.bfloat16), values, preferred_element_type=jnp.float32
            )
            if peak is None:
                total, acc = part, product
            else:
                scale = jnp.exp2(peak - new_peak)
                total = total * scale + part
                acc = acc * scale + product
            peak = new_peak
        if partial:
            out_ref[:, cols] = acc
            stats[0][:, h : h + 1] = peak
            stats[1][:, h : h + 1] = total
        else:
            result = (acc / total).astype(out_ref.dtype)
            out_ref[:, cols] = result
            if singles:
                singles[h][...] = result


def attention(place, bias, own, others, q_all, held, rows, half, total_rows, low, cols):
    group = len(own)
    partial = q_all is not None
    wide = jax.ShapeDtypeStruct((total_rows, cols), jnp.float32 if partial else jnp.bfloat16)
    thin = jax.ShapeDtypeStruct((total_rows, cols // HD), jnp.float32)
    body = functools.partial(
        attention_body,
        rows=rows,
        half=half,
        heads=cols // HD,
        low=low,
        inner=max(group // 2, 1),
        outer=total_rows // (group * rows),
        group=group,
        partial=partial,
        held=len(held),
    )
    operands = (*own, *others) + ((q_all,) if partial else ()) + held
    single = jax.ShapeDtypeStruct((total_rows, HD), jnp.bfloat16)
    heads = cols // HD
    outs = (wide, thin, thin) if partial else (wide,) + (single,) * (heads if heads > 1 else 0)
    return pl.pallas_call(
        body,
        out_shape=outs,
        in_specs=[SMEM] + [VMEM] * (1 + len(operands)),
        out_specs=(VMEM,) * len(outs),
        scratch_shapes=[pltpu.VMEM((total_rows, cols), jnp.bfloat16)],
        compiler_params=pltpu.CompilerParams(vmem_limit_bytes=VMEM_LIMIT),
        name="attend",
    )(place, bias, *operands)


def project_body(place, weight, *rest, rows, last, first):
    count = len(rows)
    parts, rest = rest[:count], rest[count:]
    left = jnp.concatenate([part[...] for part in parts], axis=1)
    right = jnp.concatenate(
        [
            weight[pl.ds(pl.multiple_of((place[0] ^ step) * width + low, HD), part.shape[1]), :]
            for part, (step, low, width) in zip(parts, rows)
        ],
        axis=0,
    )
    acc = jnp.dot(left, right, preferred_element_type=jnp.float32)
    if not first:
        acc = acc + rest[0][...]
        rest = rest[1:]
    if last:
        gate, out = rest
        acc = acc * gate[pl.ds(place[2] % 8, 1), :]
    else:
        (out,) = rest
    out[...] = acc.astype(out.dtype)


def project(place, entries, weight, before, gate, width):
    parts = [part for part, _, _ in entries]
    rows = tuple((step, low, width) for _, step, low in entries)
    first, last = before is None, gate is not None
    operands = [weight, *parts]
    operands += [] if first else [before]
    operands += [gate] if last else []
    shape = (parts[0].shape[0], weight.shape[1])
    return pl.pallas_call(
        functools.partial(project_body, rows=rows, last=last, first=first),
        out_shape=jax.ShapeDtypeStruct(shape, jnp.bfloat16 if last else jnp.float32),
        in_specs=[SMEM] + [VMEM] * len(operands),
        out_specs=VMEM,
        compiler_params=pltpu.CompilerParams(vmem_limit_bytes=VMEM_LIMIT),
        name="project",
    )(place, *operands)


def bias_body(place, mask, out, *, group, rows, half, history_rows):
    block_count = out.shape[0]
    fresh, history = group * rows, group * half
    member, core, base, live_limit = place[0], place[1], place[3], place[4]

    def positions(count, size, offset):
        column = lax.broadcasted_iota(jnp.int32, (1, count * group), 1)
        position = column
        for step in range(group):
            start = (base + (member ^ step)) * size + offset - step * count
            position = jnp.where(column >= step * count, column + start, position)
        return position

    def put(row, low, allowed):
        out[row, :, low : low + allowed.shape[1]] = jnp.where(allowed > 0, 0.0, NEGATIVE)

    position = positions(rows, rows, 0)
    for row in range(block_count):
        for low, first in ((0, block_count), (fresh, 0)):
            allowed = jnp.zeros(position.shape, jnp.int32)
            for block in range(block_count):
                within = (position >= block * BLK) & (position < (block + 1) * BLK)
                allowed = jnp.where(within, mask[row, first + block], allowed)
            put(row, low, allowed)
    for low, which in ((2 * fresh, core), (2 * fresh + history, 1 - core)):
        position = positions(half, history_rows, which * half)
        allowed = jnp.where(position < live_limit, 1, 0)
        for row in range(block_count):
            put(row, low, allowed)


def key_bias(place, block_mask, group, rows, half, history_rows):
    keys = 2 * group * (rows + half)
    return pl.pallas_call(
        functools.partial(
            bias_body, group=group, rows=rows, half=half, history_rows=history_rows
        ),
        out_shape=jax.ShapeDtypeStruct((block_mask.shape[0], 1, keys), jnp.float32),
        in_specs=[SMEM, SMEM],
        out_specs=VMEM,
        compiler_params=pltpu.CompilerParams(vmem_limit_bytes=VMEM_LIMIT),
        name="bias",
    )(place, block_mask)


def on_device(
    query, stretch_kv, history_kv, block_mask, noise_level, history_blocks, out_weight, gate_table
):
    tp_count = lax.axis_size("tp")
    tp_index = lax.axis_index("tp")
    core = lax.axis_index("stretch")
    rows = query.shape[1]
    feature_width = query.shape[2]
    history_rows = history_kv.shape[1]
    half = history_rows // 2
    group = head_groups(feature_width // HD, tp_count)
    outer = tp_count // group
    width = feature_width // group
    total_rows = tp_count * rows
    member = tp_index % group
    kv_rows = 2 * half + 2 * rows
    place = [member, core, noise_level[0], tp_index - member, history_blocks[0] * BLK]
    place = jnp.stack(place).astype(jnp.int32)
    same = [[o * group + m for o in range(outer)] for m in range(group)]
    chunks = [(low * HD, count * HD) for low, count in head_chunks(width // HD, CHUNKS)]

    bias = key_bias(place, block_mask[0], group, rows, half, history_rows)

    inner = max(group // 2, 1)
    cross = list(range(group - 1, inner - 1, -1))
    arrays = (query[0], stretch_kv[:, 0], history_kv)
    plan = [(step, low, cols) for low, cols in chunks[:1] for step in cross]
    blocks = pack(*arrays, width, plan, group) if plan else ()
    rest = [(step, 0, width) for step in range(inner)]
    rest += [(step, low, cols) for low, cols in chunks[1:] for step in cross]
    gate_rows, *others = pack(*arrays, width, rest, group, place, gate_table)
    blocks = list(blocks) + others
    plan += rest
    sends = [{} for _ in chunks]
    near = {}
    for (step, low, cols), block in zip(plan, blocks):
        if step >= inner:
            index = [first for first, _ in chunks].index(low)
            sends[index][step] = xor_permute(block, group, step)
        elif step == 0:
            near[step] = block
        else:
            near[step] = xor_permute(block, group, step)
    other_near = partner_core(
        jnp.concatenate([near[step][:kv_rows] for step in range(inner)], axis=0)
    )

    held = (out_weight, stage(out_weight))
    groups = [[] for _ in range(len(chunks) + 1)]
    for index, (low, cols) in enumerate(chunks):
        far = sends[index]
        own = [near[step] for step in range(inner)] + [far[step] for step in reversed(cross)]
        others = [other_near]
        if cross:
            others.append(
                partner_core(
                    jnp.concatenate([far[step][:kv_rows] for step in reversed(cross)], axis=0)
                )
            )
        attend = functools.partial(
            attention,
            place,
            bias,
            own,
            others,
            held=held,
            rows=rows,
            half=half,
            total_rows=total_rows,
            low=low,
            cols=cols,
        )
        if outer > 1:
            q = jnp.stack(
                [
                    block[kv_rows:, low : low + cols] if step < inner else block[kv_rows:]
                    for step, block in enumerate(own)
                ]
            )
            q = lax.all_gather(q, "tp", axis=0, axis_index_groups=same)
            out, peak, total = attend(q_all=q)
            outs, peaks, totals = (
                lax.all_gather(value, "tp", axis=0, axis_index_groups=same)
                for value in (out, peak, total)
            )
            factor = jnp.exp2(peaks - jnp.max(peaks, axis=0, keepdims=True))
            total = jnp.sum(totals * factor, axis=0)
            outs = outs.reshape(outer, total_rows, -1, HD) * factor[..., None]
            attended = (jnp.sum(outs, axis=0) / total[..., None]).astype(jnp.bfloat16)
            attended = attended.reshape(total_rows, -1)
            singles = [attended[:, at : at + HD] for at in range(0, cols, HD)]
        else:
            attended, *singles = attend(q_all=None)
            singles = singles or [attended]
        close, distant = spread(attended, singles, group, index == len(chunks) - 1)
        groups[index] += [(value, step, low) for value, step in close]
        for head, pieces in enumerate(distant):
            for number, (value, step) in enumerate(pieces):
                ended = number == len(pieces) - 1
                late = len(chunks) if ended and index >= len(chunks) - 2 else index + 1
                late = late if ended else min(late, len(chunks) - 1)
                groups[late].append((value, step, low + head * HD))

    groups = [entries for entries in groups if entries]
    result = None
    for index, entries in enumerate(groups):
        gate = gate_rows if index == len(groups) - 1 else None
        result = project(place, entries, out_weight, result, gate, width)
    return result[None]


def solution(mesh):
    return jax.shard_map(
        on_device,
        mesh=mesh,
        in_specs=(
            P(("rep", "stretch"), "tp", None),
            P(None, ("rep", "stretch"), "tp", None),
            P(None, ("rep", "tp"), None),
            P(("rep", "stretch"), None, None),
            P(("rep", "stretch")),
            P("rep"),
            P(None, "tp"),
            P(None, "tp"),
        ),
        out_specs=P(("rep", "stretch"), None, "tp"),
        check_vma=False,
    )
```
